32 devices in a mesh: section: 4 (over y, core), tp: 8 (over z, x).
Axes of the slice: x: 2, y: 2, z: 4, core: 2. Of those that a mesh axis runs over, the one named last changes fastest.
Arguments:
- embedded: bfloat16 [384, 4096], P('tp'), may hold values from -20 to 20
- previous_out: bfloat16 [4, 384, 4096], P('section', 'tp'), may hold values from -20 to 20
- top_grad: bfloat16 [384, 4096], P('tp'), may hold values from -6 to 6
- grad_out: bfloat16 [4, 384, 4096], P('section', 'tp'), may hold values from -6 to 6
- saved_input: bfloat16 [4, 384, 4096], P('section', 'tp'), may hold values from -20 to 20
- saved_qkv: bfloat16 [4, 384, 3, 2048], P('section', None, None, 'tp'), may hold values from -64 to 64
- norm_gain: float32 [4, 2, 4096], P('section'), may hold values from 0.1 to 1.9
- qkv_weight: bfloat16 [4, 2, 4096, 3, 2048], P('section', None, None, None, 'tp'), may hold values from -4 to 4
- out_weight: bfloat16 [4, 2, 2048, 4096], P('section', None, 'tp'), may hold values from -0.125 to 0.125
- modality: int32 [4, 2, 384], P('section'), may hold values from 0 to 1, as said below
- documents: int32 [4, 2, 384], P('section'), may hold values from 0 to 3, never falling along the last dimension, each value on 1 to 192 neighbouring positions
Outputs:
- forward_out: bfloat16 [4, 384, 4096], P('section', 'tp')
- backward_out: bfloat16 [4, 384, 4096], P('section', 'tp')
The draws below stay inside these ranges and needn't reach their ends.
Inputs may be any that keep to these rules, and one draw needn't show every extreme that they name: `modality`: 0 marks a text token and 1 an image token; image tokens come in runs of positions, and both modalities occur in every micro-batch. `documents`: document numbers start at 0 and never fall along the positions of a micro-batch.
All inputs are finite; a program needn't handle non-finite values.
Results may differ from the reference program's by a relative error of at most 0.014.
Values may be sent and summed in bfloat16 or wider, within the bound.
A program may use at most 128 MiB of HBM per device.

```python
import math
import jax
import jax.numpy as jnp
import numpy as np
from jax import lax

D = 4096
HEADS = 16
HEAD_DIM = 128
SECTIONS = 4
TOKENS = 384
N_TP = 8


def activation_draw(key, shape):
    rows_key, columns_key, noise_key = jax.random.split(key, 3)
    leading = shape[:-1] + (1,)
    width = shape[-1]
    row_scale = jnp.exp(jax.random.uniform(rows_key, leading, jnp.float32, math.log(0.2), math.log(2.0)))
    column_scale = jnp.exp(jax.random.uniform(columns_key, (width,), jnp.float32, math.log(0.25), math.log(2.5)))
    base = jnp.clip(jax.random.normal(noise_key, shape, jnp.float32), -4.0, 4.0)
    return (base * row_scale * column_scale).astype(jnp.bfloat16)


def draw_embedded(key, part):
    return activation_draw(jax.random.fold_in(key, 11), (TOKENS, D))


def draw_previous_out(key, part):
    return activation_draw(jax.random.fold_in(key, 12), (SECTIONS, TOKENS, D))


def draw_saved_input(key, part):
    return activation_draw(jax.random.fold_in(key, 13), (SECTIONS, TOKENS, D))


def draw_saved_qkv(key, part):
    first_key, second_key, third_key = jax.random.split(jax.random.fold_in(key, 14), 3)
    shape = (SECTIONS, TOKENS, HEADS * HEAD_DIM)
    queries = jnp.clip(jax.random.normal(first_key, shape, jnp.float32), -4.0, 4.0)
    keys = jnp.clip(jax.random.normal(second_key, shape, jnp.float32), -4.0, 4.0)
    values = jnp.clip(jax.random.normal(third_key, shape, jnp.float32), -4.0, 4.0)
    return jnp.stack([queries, keys, values], axis=2).astype(jnp.bfloat16)


def draw_qkv_weight(key, part):
    first_key, second_key, third_key = jax.random.split(jax.random.fold_in(key, 15), 3)
    shape = (SECTIONS, 2, D, HEADS * HEAD_DIM)
    spread = D ** (-0.5)
    queries = jnp.clip(jax.random.normal(first_key, shape, jnp.float32), -4.0, 4.0) * spread
    noise = jnp.clip(jax.random.normal(second_key, shape, jnp.float32), -4.0, 4.0) * spread
    values = jnp.clip(jax.random.normal(third_key, shape, jnp.float32), -4.0, 4.0) * spread
    keys = noise
    return jnp.stack([queries, keys, values], axis=3).astype(jnp.bfloat16)


def draw_modality(key, part):
    start_key, length_key = jax.random.split(jax.random.fold_in(key, 16), 2)
    starts = jax.random.randint(start_key, (SECTIONS, 2, 3), 0, TOKENS)
    spans = jax.random.randint(length_key, (SECTIONS, 2, 3), max(TOKENS // 16, 1), TOKENS // 4 + 1)
    position = jnp.arange(TOKENS, dtype=jnp.int32)
    inside = (position >= starts[..., None]) & (position < starts[..., None] + spans[..., None])
    return jnp.any(inside, axis=2).astype(jnp.int32)


def block_scale(stream_key, extent, cuts, smallest, high):
    gain = 1.0
    for dim, shards_of in cuts:
        heights = jax.random.uniform(jax.random.fold_in(jax.random.fold_in(stream_key, 6), dim), (shards_of,), jnp.float32, smallest / len(cuts), high / len(cuts))
        gain = gain * jnp.repeat(jnp.exp(heights), extent[dim] // shards_of).reshape((-1,) + (1,) * (len(extent) - 1 - dim))
    return gain


def profile(number_of, total, bound, skew):
    portions = [(1 << 20) // math.isqrt(grade ** skew) + 1 for grade in range(2, number_of + 1)]
    rest, holding = total - bound - (number_of - 1), [1] * (number_of - 1)
    while rest > 0:
        movable = [i for i in range(number_of - 1) if holding[i] < bound]
        whole, budget = sum([portions[i] for i in movable]), rest
        for i in movable:
            extra = min(bound - holding[i], max(1, budget * portions[i] // whole), rest)
            holding[i] = holding[i] + extra
            rest = rest - extra
    return np.array([bound] + holding)


def uneven_parts(rng, count, total, reach, skew):
    if count == 2:
        one = jax.random.randint(rng, (), max(1, total - reach), min(reach, total - 1) + 1)
        return jnp.stack([one, total - one])
    tallies = jnp.asarray(profile(count, total, reach, skew), jnp.int32)
    couples = (count - 1) // 2
    donor, receiver = tallies[1:1 + 2 * couples:2], tallies[2:2 + 2 * couples:2]
    margin = jnp.minimum(donor - 1, reach - receiver)
    shifted = jax.random.randint(jax.random.fold_in(rng, 1), (couples,), 0, 1 << 20) % (margin + 1)
    tallies = tallies.at[1:1 + 2 * couples:2].set(donor - shifted).at[2:2 + 2 * couples:2].set(receiver + shifted)
    return tallies[jax.random.permutation(jax.random.fold_in(rng, 2), count)]


def gaussian(stream_key, extent, scale, limit, shards=(), held_as=jnp.bfloat16):
    entries = jax.random.normal(stream_key, extent, jnp.float32) * scale
    if len(shards) > 0:
        entries = block_scale(stream_key, extent, shards, -0.22, 0.18) * entries
    return jnp.clip(entries, min=-limit, max=limit).astype(held_as)


def setup_inputs(seed: int = 0) -> dict:
    seeds = jax.random.split(jax.random.key(seed), 12)
    return {
        "embedded": draw_embedded(jax.random.fold_in(seeds[11], 71), 0),
        "previous_out": draw_previous_out(jax.random.fold_in(seeds[11], 71), 0),
        "top_grad": gaussian(seeds[2], (TOKENS, D), 1.0, 6.0, ((0, 8),)),
        "grad_out": gaussian(seeds[3], (SECTIONS, TOKENS, D), 1.0, 6.0, ((0, 4), (1, 8))),
        "saved_input": draw_saved_input(jax.random.fold_in(seeds[11], 71), 0),
        "saved_qkv": draw_saved_qkv(jax.random.fold_in(seeds[11], 71), 0),
        "norm_gain": jnp.clip(1.0 + 0.18 * jax.random.normal(seeds[6], (SECTIONS, 2, D), jnp.float32), 0.1, 1.9),
        "qkv_weight": draw_qkv_weight(jax.random.fold_in(seeds[11], 71), 0),
        "out_weight": gaussian(seeds[8], (SECTIONS, 2, HEADS * HEAD_DIM, D), (HEADS * HEAD_DIM) ** -0.5, 0.125, ((0, 4), (2, 8))),
        "modality": draw_modality(jax.random.fold_in(seeds[11], 71), 0),
        "documents": jax.vmap(lambda own: jnp.searchsorted(jnp.cumsum(uneven_parts(own, 4, TOKENS, TOKENS // 2, 0)), jnp.arange(TOKENS), side="right"))(jax.random.split(seeds[10], SECTIONS * 2)).reshape((SECTIONS, 2, TOKENS)).astype(jnp.int32),
    }


EPSILON = 1e-05

def by_modality(rows, labels, weights, side):
    numbers = (((1,), (side,)), ((), ()))
    first = lax.dot_general(rows, weights[0], numbers, preferred_element_type=jnp.float32)
    second = lax.dot_general(rows, weights[1], numbers, preferred_element_type=jnp.float32)
    return jnp.where(labels[:, None] == 0, first, second)

def gain_rows(gains, labels):
    return jnp.where(labels[:, None] == 0, gains[0][None, :], gains[1][None, :])

def probabilities(queries, keys, documents_row):
    length = queries.shape[0]
    scores = jnp.einsum('thd,shd->hts', queries.astype(jnp.float32), keys.astype(jnp.float32)) / math.sqrt(HEAD_DIM)
    position = jnp.arange(length, dtype=jnp.int32)
    allowed = (position[None, :] <= position[:, None]) & (documents_row[:, None] == documents_row[None, :])
    scores = jnp.where(allowed[None, :, :], scores, -jnp.inf)
    highest = lax.optimization_barrier(jnp.max(scores, axis=-1, keepdims=True))
    weights = jnp.exp(scores - highest)
    return weights / lax.optimization_barrier(jnp.sum(weights, axis=-1, keepdims=True))

def one_section(items):
    inputs, upstream, saved_rows, saved, gains, w_project, w_output, labels, documents_pair = items
    length = inputs.shape[0]
    group = HEADS * HEAD_DIM // N_TP
    labels_fwd = labels[0]
    labels_back = labels[1]
    forward_rows = inputs.astype(jnp.float32)
    inverse = lax.rsqrt(lax.optimization_barrier(jnp.mean(forward_rows * forward_rows, axis=-1, keepdims=True)) + EPSILON)
    normed = (forward_rows * inverse * gain_rows(gains, labels_fwd)).astype(jnp.bfloat16)
    flat_weight = w_project.reshape(2, D, 3 * HEADS * HEAD_DIM)
    projected = lax.optimization_barrier(by_modality(normed, labels_fwd, flat_weight, 0).astype(jnp.bfloat16))
    projected = projected.reshape(length, 3, HEADS, HEAD_DIM)
    probs = lax.optimization_barrier(probabilities(projected[:, 0], projected[:, 1], documents_pair[0]).astype(jnp.bfloat16))
    attended = jnp.einsum('hts,shd->thd', probs.astype(jnp.float32), projected[:, 2].astype(jnp.float32))
    attended = attended.astype(jnp.bfloat16).reshape(length, HEADS * HEAD_DIM)

    def add_output(index, total):
        begin = (index * group).astype(jnp.int32)
        rows = lax.dynamic_slice_in_dim(attended, begin, group, 1)
        weights = lax.dynamic_slice_in_dim(w_output, begin, group, 1)
        term = by_modality(rows, labels_fwd, weights, 0)
        return total + lax.optimization_barrier(term.astype(jnp.bfloat16)).astype(jnp.float32)
    mixed = lax.fori_loop(0, N_TP, add_output, jnp.zeros((length, D), jnp.float32))
    forward_out = (forward_rows + mixed).astype(jnp.bfloat16)
    grad_attended = lax.optimization_barrier(by_modality(upstream, labels_back, w_output, 1).astype(jnp.bfloat16))
    grad_attended = grad_attended.astype(jnp.float32).reshape(length, HEADS, HEAD_DIM)
    stored = saved.reshape(length, 3, HEADS, HEAD_DIM)
    queries = stored[:, 0].astype(jnp.float32)
    keys = stored[:, 1].astype(jnp.float32)
    values = stored[:, 2].astype(jnp.float32)
    probs_back = probabilities(stored[:, 0], stored[:, 1], documents_pair[1])
    rounded = lax.optimization_barrier(probs_back.astype(jnp.bfloat16)).astype(jnp.float32)
    grad_values = jnp.einsum('hts,thd->shd', rounded, grad_attended).astype(jnp.bfloat16)
    grad_probs = jnp.einsum('thd,shd->hts', grad_attended, values)
    delta = lax.optimization_barrier(jnp.sum(probs_back * grad_probs, axis=-1, keepdims=True))
    grad_scores = lax.optimization_barrier((probs_back * (grad_probs - delta) / math.sqrt(HEAD_DIM)).astype(jnp.bfloat16))
    grad_scores = grad_scores.astype(jnp.float32)
    grad_queries = jnp.einsum('hts,shd->thd', grad_scores, keys).astype(jnp.bfloat16)
    grad_keys = jnp.einsum('hts,thd->shd', grad_scores, queries).astype(jnp.bfloat16)
    grads = jnp.stack([grad_queries, grad_keys, grad_values], axis=1).reshape(length, 3, HEADS * HEAD_DIM)

    def add_input(index, total):
        begin = (index * group).astype(jnp.int32)
        rows = lax.dynamic_slice_in_dim(grads, begin, group, 2).reshape(length, 3 * group)
        weights = lax.dynamic_slice_in_dim(w_project, begin, group, 3).reshape(2, D, 3 * group)
        term = by_modality(rows, labels_back, weights, 1)
        return total + lax.optimization_barrier(term.astype(jnp.bfloat16)).astype(jnp.float32)
    grad_normed = lax.fori_loop(0, N_TP, add_input, jnp.zeros((length, D), jnp.float32))
    back_rows = saved_rows.astype(jnp.float32)
    inverse_back = lax.rsqrt(lax.optimization_barrier(jnp.mean(back_rows * back_rows, axis=-1, keepdims=True)) + EPSILON)
    scaled = grad_normed * gain_rows(gains, labels_back)
    correction = lax.optimization_barrier(jnp.mean(scaled * back_rows, axis=-1, keepdims=True))
    norm_grad = inverse_back * scaled - back_rows * inverse_back * inverse_back * inverse_back * correction
    backward_out = (upstream.astype(jnp.float32) + norm_grad).astype(jnp.bfloat16)
    return (forward_out, backward_out)

def reference(embedded, previous_out, top_grad, grad_out, saved_input, saved_qkv, norm_gain, qkv_weight, out_weight, modality, documents):
    inputs = jnp.concatenate([embedded[None], previous_out[:-1]], axis=0)
    upstream = jnp.concatenate([grad_out[1:], top_grad[None]], axis=0)
    forward_out, backward_out = lax.map(one_section, (inputs, upstream, saved_input, saved_qkv, norm_gain, qkv_weight, out_weight, modality, documents))
    return (forward_out, backward_out)
```

```python
import functools
import math

import jax
import jax.numpy as jnp
from jax import lax
from jax.experimental import pallas as pl
from jax.experimental.pallas import tpu as pltpu
from jax.sharding import PartitionSpec as P

HEAD_DIM = 128
EPSILON = 1e-05
NT = (((1,), (1,)), ((), ()))
NN = (((1,), (0,)), ((), ()))
TN = (((0,), (0,)), ((), ()))
F32 = jnp.float32
BF16 = jnp.bfloat16


def dot(a, b, dims):
    return lax.dot_general(a, b, dims, preferred_element_type=F32)


def pick(labels, first, second):
    return jnp.where(jnp.broadcast_to(labels, first.shape) == 0, first, second)


def kernel(
    n,
    sections,
    emb,
    prev,
    top,
    gout,
    saved_in,
    sqkv,
    gain,
    wq,
    wo,
    meta,
    docs,
    out_f,
    out_b,
    wq_v,
    wo_v,
    arrived,
    returned,
    xin,
    ag,
    part,
    rs,
    acc,
    pr,
    att,
    grads,
    w_sem,
    sec_send,
    sec_recv,
    ag_send,
    ag_recv,
    rs_send,
    rs_recv,
):
    half = n // 2
    local, width = emb.shape
    cols = width // 2
    length = n * local
    hw = wo.shape[1]
    heads = hw // HEAD_DIM
    scale = 1.0 / math.sqrt(HEAD_DIM)
    section = lax.axis_index("section")
    me = lax.axis_index("tp")
    odd = me % 2
    pos = (1 - odd) * (me // 2) + odd * (n - 1 - me // 2)

    def member(p):
        q = (p + 2 * n) % n
        upper = q // half
        return (1 - upper) * 2 * q + upper * (2 * (n - q) - 1)

    neighbours = ({"tp": member(pos + 1)}, {"tp": member(pos - 1)})
    after = {"section": (section + 1) % sections}
    before = {"section": (section + sections - 1) % sections}

    w_copies = [
        pltpu.make_async_copy(wq, wq_v, w_sem.at[0]),
        pltpu.make_async_copy(wo, wo_v, w_sem.at[1]),
    ]
    for c in w_copies:
        c.start()

    barrier = pltpu.get_barrier_semaphore()
    for device in (*neighbours, after, before):
        pl.semaphore_signal(
            barrier, inc=1, device_id=device, device_id_type=pl.DeviceIdType.MESH
        )
    pl.semaphore_wait(barrier, 4)

    def remote(src, dst, send, recv, device):
        return pltpu.make_async_remote_copy(
            src_ref=src,
            dst_ref=dst,
            send_sem=send,
            recv_sem=recv,
            device_id=device,
            device_id_type=pl.DeviceIdType.MESH,
        )

    hand_f = remote(prev, arrived, sec_send.at[0], sec_recv.at[0], after)
    hand_b = remote(gout, returned, sec_send.at[1], sec_recv.at[1], before)
    hand_f.start()
    hand_b.start()
    sent = []

    def chunk(c):
        return pl.ds(c * cols, cols)

    def ag_chunks(d, k):
        return (0, 1) if k < half else (d,)

    def ag_copy(p, d, k, c):
        sign = 1 - 2 * d
        block = ag.at[p, member(pos - sign * (k - 1)), :, chunk(c)]
        return remote(
            block, block, ag_send.at[p, d, k - 1, c], ag_recv.at[p, d, k - 1, c], neighbours[d]
        )

    def ag_step(p, k):
        for c in range(2):
            for d in range(2):
                if k > 1 and c in ag_chunks(d, k - 1):
                    ag_copy(p, d, k - 1, c).wait_recv()
                if k <= half and c in ag_chunks(d, k):
                    copy = ag_copy(p, d, k, c)
                    copy.start()
                    sent.append(copy)

    def rs_chunks(d, k):
        return (0, 1) if k > 1 else (d,)

    def rs_copy(p, d, k, c):
        sign = 1 - 2 * d
        if k > 1 and c in rs_chunks(d, k - 1):
            src = rs.at[p, d, k - 2, :, chunk(c)]
        else:
            src = part.at[p, member(pos + sign * (half + 1 - k)), :, chunk(c)]
        dst = rs.at[p, d, k - 1, :, chunk(c)]
        return remote(
            src, dst, rs_send.at[p, d, k - 1, c], rs_recv.at[p, d, k - 1, c], neighbours[d]
        )

    def rs_step(p, k):
        for c in range(2):
            for d in range(2):
                sign = 1 - 2 * d
                if k > 1 and c in rs_chunks(d, k - 1):
                    rs_copy(p, d, k - 1, c).wait_recv()
                    if k <= half:
                        own = part[p, member(pos + sign * (half + 1 - k)), :, chunk(c)]
                        here = rs[p, d, k - 2, :, chunk(c)]
                        rs[p, d, k - 2, :, chunk(c)] = (
                            here.astype(F32) + own.astype(F32)
                        ).astype(BF16)
                if k <= half and c in rs_chunks(d, k):
                    copy = rs_copy(p, d, k, c)
                    copy.start()
                    sent.append(copy)

    def rs_total(p):
        return (
            part[p, me].astype(F32)
            + rs[p, 0, half - 1].astype(F32)
            + rs[p, 1, half - 1].astype(F32)
        )

    def own_labels(col):
        return meta[pl.ds(pl.multiple_of(me * local, 8), local), col : col + 1]

    def gains(col):
        labels = jnp.broadcast_to(own_labels(col), (local, width))
        return jnp.where(labels == 0, gain[0:1, :], gain[1:2, :])

    def probabilities(queries, keys, which):
        scores = dot(queries, keys, NT) * scale
        row = lax.broadcasted_iota(jnp.int32, (length, length), 0)
        column = lax.broadcasted_iota(jnp.int32, (length, length), 1)
        allowed = (column <= row) & (meta[:, 2 + which : 3 + which] == docs[which : which + 1, :])
        scores = jnp.where(allowed, scores, -jnp.inf)
        weights = jnp.exp(scores - jnp.max(scores, axis=-1, keepdims=True))
        return weights / jnp.sum(weights, axis=-1, keepdims=True)

    depth = min(1024, width)

    def project(p, weights, dims):
        acc[...] = jnp.zeros_like(acc)

        def step(i, carry):
            at = pl.ds(pl.multiple_of(i * depth, depth), depth)
            rows = ag[p, :, :, at].reshape(length, depth)
            for m in range(2):
                acc[m] += dot(rows, weights(m, at), dims)
            return carry

        lax.fori_loop(0, width // depth, step, 0)
        return pick(meta[:, p : p + 1], acc[0], acc[1]).astype(BF16)

    def project_qkv(j):
        pr[j] = project(0, lambda m, at: wq_v[m, j, at, :], NN)

    def attend():
        for h in range(heads):
            at = pl.ds(h * HEAD_DIM, HEAD_DIM)
            probs = probabilities(pr[0, :, at], pr[1, :, at], 0).astype(BF16)
            att[:, at] = dot(probs, pr[2, :, at], NN).astype(BF16)

    tile = 256

    def spread(p, term, first, last):
        def step(i, carry):
            at = pl.ds(pl.multiple_of(i * tile, tile), tile)
            both = [term(m, at) for m in range(2)]
            block = pick(meta[:, p : p + 1], *both).astype(BF16)
            part[p, :, :, at] = block.reshape(n, local, tile)
            return carry

        lax.fori_loop(first, last, step, 0)

    def forward_terms():
        spread(0, lambda m, at: dot(att[...], wo_v[m, :, at], NN), 0, width // tile)

    def backward_term(m, at):
        total = dot(grads[0], wq_v[m, 0, at, :], NT)
        for j in (1, 2):
            total += dot(grads[j], wq_v[m, j, at, :], NT)
        return total

    def backward_terms(first, last):
        spread(1, backward_term, first, last)

    def grad_attended():
        att[...] = project(1, lambda m, at: wo_v[m, :, at], NT)

    def backward_head(h):
        at = pl.ds(h * HEAD_DIM, HEAD_DIM)
        queries, keys, values = (sqkv[j, :, at] for j in range(3))
        upstream = att[:, at]
        probs = probabilities(queries, keys, 1)
        grads[2, :, at] = dot(probs.astype(BF16), upstream, TN).astype(BF16)
        grad_probs = dot(upstream, values, NT)
        delta = jnp.sum(probs * grad_probs, axis=-1, keepdims=True)
        grad_scores = (probs * (grad_probs - delta) * scale).astype(BF16)
        grads[0, :, at] = dot(grad_scores, keys, NN).astype(BF16)
        grads[1, :, at] = dot(grad_scores, queries, TN).astype(BF16)

    def interleave(pieces, steps):
        done = 0
        for i, piece in enumerate(pieces):
            piece()
            due = (i + 1) * len(steps) // len(pieces)
            for s in steps[done:due]:
                s()
            done = due

    hand_f.wait_recv()
    rows = jnp.where(section == 0, emb[...], arrived[...])
    xin[...] = rows
    rows = rows.astype(F32)
    inverse = lax.rsqrt(jnp.mean(rows * rows, axis=-1, keepdims=True) + EPSILON)
    ag[0, me] = (rows * inverse * gains(0)).astype(BF16)
    ag_step(0, 1)
    hand_b.wait_recv()
    ag[1, me] = jnp.where(section == sections - 1, top[...], returned[...])
    for k in range(2, half + 1):
        ag_step(0, k)
    ag_step(1, 1)
    ag_step(0, half + 1)
    for c in w_copies:
        c.wait()

    interleave(
        [functools.partial(project_qkv, j) for j in range(3)] + [attend, forward_terms],
        [functools.partial(ag_step, 1, k) for k in range(2, half + 1)],
    )
    rs_step(0, 1)
    ag_step(1, half + 1)
    tiles = width // tile
    interleave(
        [grad_attended]
        + [functools.partial(backward_head, h) for h in range(heads)]
        + [
            functools.partial(backward_terms, 0, tiles // 2),
            functools.partial(backward_terms, tiles // 2, tiles),
        ],
        [functools.partial(rs_step, 0, k) for k in range(2, half + 1)],
    )
    rs_step(1, 1)
    rs_step(0, half + 1)
    out_f[...] = (xin[...].astype(F32) + rs_total(0)).astype(BF16)
    for k in range(2, half + 2):
        rs_step(1, k)
    back_rows = saved_in[...].astype(F32)
    inverse = lax.rsqrt(jnp.mean(back_rows * back_rows, axis=-1, keepdims=True) + EPSILON)
    scaled = rs_total(1) * gains(1)
    correction = jnp.mean(scaled * back_rows, axis=-1, keepdims=True)
    norm_grad = inverse * scaled - back_rows * (inverse * inverse * inverse * correction)
    out_b[...] = (ag[1, me].astype(F32) + norm_grad).astype(BF16)

    hand_f.wait_send()
    hand_b.wait_send()
    for copy in sent:
        copy.wait_send()


def body(
    n,
    sections,
    embedded,
    previous_out,
    top_grad,
    grad_out,
    saved_input,
    saved_qkv,
    norm_gain,
    qkv_weight,
    out_weight,
    modality,
    documents,
):
    local, width = embedded.shape
    length = local * n
    hw = out_weight.shape[2]
    half = n // 2
    meta = jnp.concatenate([modality[0], documents[0]], axis=0).T
    vmem = pl.BlockSpec(memory_space=pltpu.VMEM)
    hbm = pl.BlockSpec(memory_space=pl.ANY)
    dma = pltpu.SemaphoreType.DMA
    out = jax.ShapeDtypeStruct((local, width), BF16)
    forward_out, backward_out = pl.pallas_call(
        functools.partial(kernel, n, sections),
        out_shape=(out, out),
        in_specs=[vmem] * 7 + [hbm, hbm] + [vmem] * 2,
        out_specs=(vmem, vmem),
        scratch_shapes=[
            pltpu.VMEM((2, 3, width, hw), BF16),
            pltpu.VMEM((2, hw, width), BF16),
            pltpu.VMEM((local, width), BF16),
            pltpu.VMEM((local, width), BF16),
            pltpu.VMEM((local, width), BF16),
            pltpu.VMEM((2, n, local, width), BF16),
            pltpu.VMEM((2, n, local, width), BF16),
            pltpu.VMEM((2, 2, half, local, width), BF16),
            pltpu.VMEM((2, length, hw), F32),
            pltpu.VMEM((3, length, hw), BF16),
            pltpu.VMEM((length, hw), BF16),
            pltpu.VMEM((3, length, hw), BF16),
            dma((2,)),
            dma((2,)),
            dma((2,)),
            dma((2, 2, half, 2)),
            dma((2, 2, half, 2)),
            dma((2, 2, half, 2)),
            dma((2, 2, half, 2)),
        ],
        compiler_params=pltpu.CompilerParams(
            collective_id=0, has_side_effects=True, vmem_limit_bytes=64000000
        ),
    )(
        embedded,
        previous_out[0],
        top_grad,
        grad_out[0],
        saved_input[0],
        saved_qkv[0].transpose(1, 0, 2),
        norm_gain[0],
        qkv_weight[0].transpose(0, 2, 1, 3),
        out_weight[0],
        meta,
        documents[0],
    )
    return (forward_out[None], backward_out[None])


def solution(mesh):
    placed = (
        P("tp", None),
        P("section", "tp", None),
        P("tp", None),
        P("section", "tp", None),
        P("section", "tp", None),
        P("section", None, None, "tp"),
        P("section", None, None),
        P("section", None, None, None, "tp"),
        P("section", None, "tp", None),
        P("section", None, None),
        P("section", None, None),
    )
    return jax.shard_map(
        functools.partial(body, mesh.shape["tp"], mesh.shape["section"]),
        mesh=mesh,
        in_specs=placed,
        out_specs=(P("section", "tp", None), P("section", "tp", None)),
        check_vma=False,
    )
```

```python
import functools
import math

import jax
import jax.numpy as jnp
from jax import lax
from jax.experimental import pallas as pl
from jax.experimental.pallas import tpu as pltpu
from jax.sharding import PartitionSpec as P

HEAD_DIM = 128
EPSILON = 1e-05
NT = (((1,), (1,)), ((), ()))
NN = (((1,), (0,)), ((), ()))
TN = (((0,), (0,)), ((), ()))
F32 = jnp.float32
BF16 = jnp.bfloat16
CHUNKS = 4


def dot(a, b, dims):
    return lax.dot_general(a, b, dims, preferred_element_type=F32)


def pick(labels, first, second):
    return jnp.where(jnp.broadcast_to(labels, first.shape) == 0, first, second)


def kernel(
    n,
    sections,
    emb,
    prev,
    top,
    gout,
    saved_in,
    sqkv,
    gain,
    wq,
    wo,
    labels,
    docs,
    out,
    wq_v,
    wo_v,
    arrived,
    returned,
    xin,
    ag,
    part,
    rs,
    acc,
    pr,
    att,
    grads,
    meta,
    w_sem,
    sec_send,
    sec_recv,
    ag_send,
    ag_recv,
    rs_send,
    rs_recv,
):
    half = n // 2
    local, width = emb.shape
    cols = width // CHUNKS
    length = n * local
    hw = wo.shape[1]
    heads = hw // HEAD_DIM
    scale = 1.0 / math.sqrt(HEAD_DIM)
    section = lax.axis_index("section")
    me = lax.axis_index("tp")
    odd = me % 2
    pos = (1 - odd) * (me // 2) + odd * (n - 1 - me // 2)

    def member(p):
        q = (p + 2 * n) % n
        upper = q // half
        return (1 - upper) * 2 * q + upper * (2 * (n - q) - 1)

    neighbours = ({"tp": member(pos + 1)}, {"tp": member(pos - 1)})
    after = {"section": (section + 1) % sections}
    before = {"section": (section + sections - 1) % sections}
    has_after = section < sections - 1
    has_before = section > 0

    w_copies = [
        pltpu.make_async_copy(wq, wq_v, w_sem.at[0]),
        pltpu.make_async_copy(wo, wo_v, w_sem.at[1]),
    ]
    for c in w_copies:
        c.start()

    barrier = pltpu.get_barrier_semaphore()
    for device in (*neighbours, after, before):
        pl.semaphore_signal(
            barrier, inc=1, device_id=device, device_id_type=pl.DeviceIdType.MESH
        )
    pl.semaphore_wait(barrier, 4)

    def remote(src, dst, send, recv, device):
        return pltpu.make_async_remote_copy(
            src_ref=src,
            dst_ref=dst,
            send_sem=send,
            recv_sem=recv,
            device_id=device,
            device_id_type=pl.DeviceIdType.MESH,
        )

    hand_f = remote(prev, arrived, sec_send.at[0], sec_recv.at[0], after)
    hand_b = remote(gout, returned, sec_send.at[1], sec_recv.at[1], before)

    @pl.when(has_after)
    def _():
        hand_f.start()

    @pl.when(has_before)
    def _():
        hand_b.start()

    line = lax.broadcasted_iota(jnp.int32, (8, length), 0)
    stacked = jnp.broadcast_to(docs[1:2, :], (8, length))
    for i, row in ((2, docs[0:1, :]), (1, labels[1:2, :]), (0, labels[0:1, :])):
        stacked = jnp.where(line == i, jnp.broadcast_to(row, (8, length)), stacked)
    meta[...] = stacked.T
    sent = []

    def chunk(c):
        return pl.ds(c * cols, cols)

    def side(d):
        return range(d * CHUNKS // 2, (d + 1) * CHUNKS // 2)

    def ag_chunks(d, k):
        return range(CHUNKS) if k < half else side(d)

    def ag_copy(p, d, k, c):
        sign = 1 - 2 * d
        block = ag.at[p, member(pos - sign * (k - 1)), :, chunk(c)]
        return remote(
            block, block, ag_send.at[p, d, k - 1, c], ag_recv.at[p, d, k - 1, c], neighbours[d]
        )

    def ag_step(p, k):
        for c in range(CHUNKS):
            for d in range(2):
                if k > 1 and c in ag_chunks(d, k - 1):
                    ag_copy(p, d, k - 1, c).wait_recv()
                if k <= half and c in ag_chunks(d, k):
                    copy = ag_copy(p, d, k, c)
                    copy.start()
                    sent.append(copy)

    def rs_chunks(d, k):
        return range(CHUNKS) if k > 1 else side(d)

    def rs_copy(p, d, k, c):
        sign = 1 - 2 * d
        if k > 1 and c in rs_chunks(d, k - 1):
            src = rs.at[p, d, k - 2, :, chunk(c)]
        else:
            src = part.at[p, member(pos + sign * (half + 1 - k)), :, chunk(c)]
        dst = rs.at[p, d, k - 1, :, chunk(c)]
        return remote(
            src, dst, rs_send.at[p, d, k - 1, c], rs_recv.at[p, d, k - 1, c], neighbours[d]
        )

    def rs_start(p, d, k, c):
        copy = rs_copy(p, d, k, c)
        copy.start()
        sent.append(copy)

    def rs_begin(p):
        for k in (1, 2):
            for i in range(CHUNKS // 2):
                for d in range(2):
                    rs_start(p, d, k, side(d if k == 1 else 1 - d)[i])

    def rs_step(p, k):
        for i in range(CHUNKS):
            for d in range(2):
                order = [*side(d), *side(1 - d)]
                c = order[i]
                if c not in rs_chunks(d, k - 1):
                    continue
                sign = 1 - 2 * d
                rs_copy(p, d, k - 1, c).wait_recv()
                if k <= half:
                    own = part[p, member(pos + sign * (half + 1 - k)), :, chunk(c)]
                    here = rs[p, d, k - 2, :, chunk(c)]
                    rs[p, d, k - 2, :, chunk(c)] = (
                        here.astype(F32) + own.astype(F32)
                    ).astype(BF16)
                    rs_start(p, d, k, c)

    def rs_total(p):
        return (
            part[p, me].astype(F32)
            + rs[p, 0, half - 1].astype(F32)
            + rs[p, 1, half - 1].astype(F32)
        )

    def own_labels(col):
        return meta[pl.ds(pl.multiple_of(me * local, 8), local), col : col + 1]

    def gains(col):
        own = jnp.broadcast_to(own_labels(col), (local, width))
        return jnp.where(own == 0, gain[0:1, :], gain[1:2, :])

    def probabilities(queries, keys, which):
        scores = dot(queries, keys, NT) * scale
        row = lax.broadcasted_iota(jnp.int32, (length, length), 0)
        column = lax.broadcasted_iota(jnp.int32, (length, length), 1)
        allowed = (column <= row) & (meta[:, 2 + which : 3 + which] == docs[which : which + 1, :])
        scores = jnp.where(allowed, scores, -jnp.inf)
        weights = jnp.exp(scores - jnp.max(scores, axis=-1, keepdims=True))
        return weights / jnp.sum(weights, axis=-1, keepdims=True)

    depth = min(1024, width)

    def project(p, weights, dims):
        acc[...] = jnp.zeros_like(acc)

        def step(i, carry):
            at = pl.ds(pl.multiple_of(i * depth, depth), depth)
            rows = ag[p, :, :, at].reshape(length, depth)
            for m in range(2):
                acc[m] += dot(rows, weights(m, at), dims)
            return carry

        lax.fori_loop(0, width // depth, step, 0)
        return pick(meta[:, p : p + 1], acc[0], acc[1]).astype(BF16)

    def project_qkv(j):
        pr[j] = project(0, lambda m, at: wq_v[m, j, at, :], NN)

    def attend():
        for h in range(heads):
            at = pl.ds(h * HEAD_DIM, HEAD_DIM)
            probs = probabilities(pr[0, :, at], pr[1, :, at], 0).astype(BF16)
            att[:, at] = dot(probs, pr[2, :, at], NN).astype(BF16)

    tile = 256

    def spread(p, term, first, last):
        def step(i, carry):
            at = pl.ds(pl.multiple_of(i * tile, tile), tile)
            both = [term(m, at) for m in range(2)]
            block = pick(meta[:, p : p + 1], *both).astype(BF16)
            part[p, :, :, at] = block.reshape(n, local, tile)
            return carry

        lax.fori_loop(first, last, step, 0)

    def forward_terms():
        spread(0, lambda m, at: dot(att[...], wo_v[m, :, at], NN), 0, width // tile)

    def backward_term(m, at):
        total = dot(grads[0], wq_v[m, 0, at, :], NT)
        for j in (1, 2):
            total += dot(grads[j], wq_v[m, j, at, :], NT)
        return total

    def backward_terms(first, last):
        spread(1, backward_term, first, last)

    def grad_attended():
        att[...] = project(1, lambda m, at: wo_v[m, :, at], NT)

    def backward_head(h):
        at = pl.ds(h * HEAD_DIM, HEAD_DIM)
        queries, keys, values = (sqkv[j, :, at] for j in range(3))
        upstream = att[:, at]
        probs = probabilities(queries, keys, 1)
        grads[2, :, at] = dot(probs.astype(BF16), upstream, TN).astype(BF16)
        grad_probs = dot(upstream, values, NT)
        delta = jnp.sum(probs * grad_probs, axis=-1, keepdims=True)
        grad_scores = (probs * (grad_probs - delta) * scale).astype(BF16)
        grads[0, :, at] = dot(grad_scores, keys, NN).astype(BF16)
        grads[1, :, at] = dot(grad_scores, queries, TN).astype(BF16)

    def interleave(pieces, steps):
        done = 0
        for i, piece in enumerate(pieces):
            piece()
            due = (i + 1) * len(steps) // len(pieces)
            for s in steps[done:due]:
                s()
            done = due

    @pl.when(has_before)
    def _():
        hand_f.wait_recv()
        xin[...] = arrived[...]

    @pl.when(section == 0)
    def _():
        xin[...] = emb[...]

    rows = xin[...]
    rows = rows.astype(F32)
    inverse = lax.rsqrt(jnp.mean(rows * rows, axis=-1, keepdims=True) + EPSILON)
    ag[0, me] = (rows * inverse * gains(0)).astype(BF16)
    ag_step(0, 1)

    @pl.when(has_after)
    def _():
        hand_b.wait_recv()
        ag[1, me] = returned[...]

    @pl.when(section == sections - 1)
    def _():
        ag[1, me] = top[...]

    for k in range(2, half + 1):
        ag_step(0, k)
    ag_step(1, 1)
    ag_step(0, half + 1)
    for c in w_copies:
        c.wait()

    interleave(
        [functools.partial(project_qkv, j) for j in range(3)] + [attend, forward_terms],
        [functools.partial(ag_step, 1, k) for k in range(2, half + 1)],
    )
    rs_begin(0)
    ag_step(1, half + 1)
    tiles = width // tile
    interleave(
        [grad_attended]
        + [functools.partial(backward_head, h) for h in range(heads)]
        + [
            functools.partial(backward_terms, 0, tiles // 2),
            functools.partial(backward_terms, tiles // 2, tiles),
        ],
        [functools.partial(rs_step, 0, k) for k in range(2, half + 1)],
    )
    rs_begin(1)
    rs_step(0, half + 1)
    out[0] = (xin[...].astype(F32) + rs_total(0)).astype(BF16)
    for k in range(2, half + 1):
        rs_step(1, k)
    back_rows = saved_in[...].astype(F32)
    inverse = lax.rsqrt(jnp.mean(back_rows * back_rows, axis=-1, keepdims=True) + EPSILON)
    rs_step(1, half + 1)
    scaled = rs_total(1) * gains(1)
    correction = jnp.mean(scaled * back_rows, axis=-1, keepdims=True)
    norm_grad = inverse * scaled - back_rows * (inverse * inverse * inverse * correction)
    out[1] = (ag[1, me].astype(F32) + norm_grad).astype(BF16)

    @pl.when(has_after)
    def _():
        hand_f.wait_send()

    @pl.when(has_before)
    def _():
        hand_b.wait_send()

    for copy in sent:
        copy.wait_send()


def body(
    n,
    sections,
    embedded,
    previous_out,
    top_grad,
    grad_out,
    saved_input,
    saved_qkv,
    norm_gain,
    qkv_weight,
    out_weight,
    modality,
    documents,
):
    local, width = embedded.shape
    length = local * n
    hw = out_weight.shape[2]
    half = n // 2
    vmem = pl.BlockSpec(memory_space=pltpu.VMEM)
    hbm = pl.BlockSpec(memory_space=pl.ANY)
    dma = pltpu.SemaphoreType.DMA
    out = jax.ShapeDtypeStruct((2, local, width), BF16)
    both = pl.pallas_call(
        functools.partial(kernel, n, sections),
        out_shape=out,
        in_specs=[vmem] * 7 + [hbm, hbm] + [vmem] * 2,
        out_specs=vmem,
        scratch_shapes=[
            pltpu.VMEM((2, 3, width, hw), BF16),
            pltpu.VMEM((2, hw, width), BF16),
            pltpu.VMEM((local, width), BF16),
            pltpu.VMEM((local, width), BF16),
            pltpu.VMEM((local, width), BF16),
            pltpu.VMEM((2, n, local, width), BF16),
            pltpu.VMEM((2, n, local, width), BF16),
            pltpu.VMEM((2, 2, half, local, width), BF16),
            pltpu.VMEM((2, length, hw), F32),
            pltpu.VMEM((3, length, hw), BF16),
            pltpu.VMEM((length, hw), BF16),
            pltpu.VMEM((3, length, hw), BF16),
            pltpu.VMEM((length, 8), jnp.int32),
            dma((2,)),
            dma((2,)),
            dma((2,)),
            dma((2, 2, half, CHUNKS)),
            dma((2, 2, half, CHUNKS)),
            dma((2, 2, half, CHUNKS)),
            dma((2, 2, half, CHUNKS)),
        ],
        compiler_params=pltpu.CompilerParams(
            collective_id=0, has_side_effects=True, vmem_limit_bytes=64000000
        ),
    )(
        embedded,
        previous_out[0],
        top_grad,
        grad_out[0],
        saved_input[0],
        saved_qkv[0].transpose(1, 0, 2),
        norm_gain[0],
        qkv_weight[0].transpose(0, 2, 1, 3),
        out_weight[0],
        modality[0],
        documents[0],
    )
    return (both[0:1], both[1:2])


def solution(mesh):
    placed = (
        P("tp", None),
        P("section", "tp", None),
        P("tp", None),
        P("section", "tp", None),
        P("section", "tp", None),
        P("section", None, None, "tp"),
        P("section", None, None),
        P("section", None, None, None, "tp"),
        P("section", None, "tp", None),
        P("section", None, None),
        P("section", None, None),
    )
    return jax.shard_map(
        functools.partial(body, mesh.shape["tp"], mesh.shape["section"]),
        mesh=mesh,
        in_specs=placed,
        out_specs=(P("section", "tp", None), P("section", "tp", None)),
        check_vma=False,
    )
```
